16 devices in a mesh: rep: 4 (over y, z, core), dp: 4 (over x).
Axes of the slice: x: 4, y: 2, z: 1, core: 2. Of those that a mesh axis runs over, the one named last changes fastest.
The devices are a block of a 4x4x8 slice.
Arguments:
- g_w_gate: bfloat16 [16, 2, 1024, 4096], P(('rep', 'dp')), parts along dimension 0
- g_w_up: bfloat16 [16, 2, 1024, 4096], P(('rep', 'dp')), parts along dimension 0
- g_w_down: bfloat16 [16, 2, 4096, 1024], P(('rep', 'dp')), parts along dimension 0
- w_gate: bfloat16 [2, 1024, 4096], replicated
- w_up: bfloat16 [2, 1024, 4096], replicated
- w_down: bfloat16 [2, 4096, 1024], replicated
- m_w_gate: float32 [2, 1024, 4096], P(None, 'dp')
- m_w_up: float32 [2, 1024, 4096], P(None, 'dp')
- m_w_down: float32 [2, 4096, 1024], P(None, 'dp')
- v_w_gate: float32 [2, 1024, 4096], P(None, 'dp')
- v_w_up: float32 [2, 1024, 4096], P(None, 'dp')
- v_w_down: float32 [2, 4096, 1024], P(None, 'dp')
Outputs:
- output 1: bfloat16 [8, 1024, 4096], P('rep'), parts along dimension 0
- output 2: bfloat16 [8, 1024, 4096], P('rep'), parts along dimension 0
- output 3: bfloat16 [8, 4096, 1024], P('rep'), parts along dimension 0
- output 4: float32 [8, 1024, 4096], P('rep', 'dp'), parts along dimension 0
- output 5: float32 [8, 1024, 4096], P('rep', 'dp'), parts along dimension 0
- output 6: float32 [8, 4096, 1024], P('rep', 'dp'), parts along dimension 0
- output 7: float32 [8, 1024, 4096], P('rep', 'dp'), parts along dimension 0
- output 8: float32 [8, 1024, 4096], P('rep', 'dp'), parts along dimension 0
- output 9: float32 [8, 4096, 1024], P('rep', 'dp'), parts along dimension 0
There are 4 independent parts. The reference program is written for one: setup_inputs(seed, part) draws one part's arguments, and reference() takes and returns one part's arrays. A program takes and returns all parts, laid end to end along the dimension named above; an argument that names none is the same for every part.
All inputs are finite; a program needn't handle non-finite values.
Results may differ from the reference program's by a relative error of at most 0.022.
Values are sent between devices in bfloat16 or wider.
A program may use at most 768 MiB of HBM per device.

```python
import jax
import jax.numpy as jnp
from jax import lax

DEVICES = 4
D = 1024
FF = 4096
LAYERS = 2
NAMES = ("w_gate", "w_up", "w_down")
SHAPES = {"w_gate": (LAYERS, D, FF), "w_up": (LAYERS, D, FF), "w_down": (LAYERS, FF, D)}


def setup_inputs(seed: int = 0, part: int = 0) -> dict:
    kz, *keys = jax.random.split(jax.random.key(seed), 1 + 5 * len(NAMES))
    loud = 2.0 ** jax.random.uniform(kz, (), jnp.float32, -1.0, 1.0)
    drawn = {}
    for name, key, both in zip(NAMES, keys[:3], keys[3:6], strict=True):
        own = jax.random.normal(jax.random.fold_in(key, part), (DEVICES, *SHAPES[name]), jnp.float32)
        shared = jax.random.normal(jax.random.fold_in(both, part), SHAPES[name], jnp.float32)
        drawn["g_" + name] = (loud * (0.7 * shared / DEVICES + 0.7 * own * DEVICES**-0.5)).astype(jnp.bfloat16)
    for name, key in zip(NAMES, keys[6:9], strict=True):
        drawn[name] = (jax.random.normal(key, SHAPES[name], jnp.float32) * SHAPES[name][1] ** -0.5).astype(jnp.bfloat16)
    for name, key in zip(NAMES, keys[9:12], strict=True):
        drawn["m_" + name] = loud * 0.5 * jax.random.normal(key, SHAPES[name], jnp.float32)
    for name, key in zip(NAMES, keys[12:15], strict=True):
        drawn["v_" + name] = loud * loud * jax.random.uniform(key, SHAPES[name], jnp.float32, 0.5, 1.5)
    return drawn


def adamw(w, m, v, g):
    m = 0.9 * m + 0.1 * g
    v = 0.95 * v + 0.05 * g * g
    step = m * lax.rsqrt(v + 1e-8) + 0.1 * w
    return (w - 0.02 * step).astype(jnp.bfloat16), m, v


def reference(g_w_gate, g_w_up, g_w_down, w_gate, w_up, w_down, m_w_gate, m_w_up, m_w_down, v_w_gate, v_w_up, v_w_down):
    def total(terms):
        return lax.scan(lambda so_far, term: (so_far + term.astype(jnp.float32), None), jnp.zeros(terms.shape[1:], jnp.float32), terms)[0]

    gradients = [total(terms).astype(jnp.bfloat16).astype(jnp.float32) for terms in (g_w_gate, g_w_up, g_w_down)]
    new = [
        adamw(w.astype(jnp.float32), m, v, g)
        for w, m, v, g in zip((w_gate, w_up, w_down), (m_w_gate, m_w_up, m_w_down), (v_w_gate, v_w_up, v_w_down), gradients, strict=True)
    ]
    return tuple(one[which] for which in range(3) for one in new)
```

```python
import functools

import jax
import jax.numpy as jnp
from jax import lax
from jax.experimental import pallas as pl
from jax.experimental.pallas import tpu as pltpu
from jax.sharding import PartitionSpec as P

MESH = pl.DeviceIdType.MESH
ROWS, COLS = 256, 1024
RIGHT, LEFT = 0, 1
STRIP = 32
LATER = 3
VMEM_LIMIT = 67043328


def adamw(w, m, v, g):
    m = 0.9 * m + 0.1 * g
    v = 0.95 * v + 0.05 * g * g
    step = m * lax.rsqrt(v + 1e-8) + 0.1 * w
    return (w - 0.02 * step).astype(jnp.bfloat16), m, v


class Pieces:
    def __init__(self, block):
        self.layers, self.rows, cols = block
        self.across = cols // COLS
        self.each = (self.rows // ROWS) * self.across
        assert self.rows % ROWS == 0 and cols % COLS == 0 and self.each % 2 == 0

    def of(self, ref, layer, owner, q):
        start = pl.multiple_of(owner * self.rows + (q // self.across) * ROWS, ROWS)
        return ref.at[layer, pl.ds(start, ROWS), pl.ds((q % self.across) * COLS, COLS)]


def kernel(lay, *refs):
    grads, weights, ms, vs, sums, gathered = (refs[i : i + 3] for i in range(0, 18, 3))
    onward = refs[18:20]
    (
        hop, got, own_b, g_b, w_b, m_b, v_b, sum_b, new_b,
        s1_send, s1_recv, s2_send, s2_recv, a1_send, a1_recv, a2_send, a2_recv,
        own_sem, in_sem, out_sem,
    ) = refs[20:]
    n = lax.axis_size("dp")
    me = lax.axis_index("dp")
    rep = lax.axis_index("rep")
    right, left, across = lax.rem(me + 1, n), lax.rem(me + n - 1, n), lax.rem(me + 2, n)
    to = (right, left)
    came = (left, right)

    units = [(i, layer) for i in range(3) for layer in range(lay[i].layers)]
    each = lay[0].each
    half = each // 2
    halves = (range(0, half), range(half, each))

    def remote(src, dst, sends, recvs, d, k):
        return pltpu.make_async_remote_copy(
            src_ref=src,
            dst_ref=dst,
            send_sem=sends.at[d, k],
            recv_sem=recvs.at[d, k],
            device_id=(rep, to[d]),
            device_id_type=MESH,
        )

    def piece(arrays, u, owner, q):
        i, layer = units[u]
        return lay[i].of(arrays[i], layer, owner, q)

    def first(d, u, j):
        return remote(piece(grads, u, across, halves[d][j]), hop.at[d, u * half + j], s1_send, s1_recv, d, u * half + j)

    def plain(d, u, j):
        q = halves[1 - d][j]
        return remote(piece(grads, u, to[d], q), got.at[d, u * each + q], s2_send, s2_recv, d, u * each + q)

    def added(d, u, j):
        q = halves[d][j]
        return remote(hop.at[d, u * half + j], got.at[d, u * each + q], s2_send, s2_recv, d, u * each + q)

    def out(d, u, q):
        src = piece(gathered, u, me, q)
        return remote(src, src, a1_send, a1_recv, d, u * each + q)

    def on(d, u, j):
        src = piece(gathered, u, came[d], halves[d][j])
        return remote(src, src, a2_send, a2_recv, d, u * half + j)

    barrier = pltpu.get_barrier_semaphore()
    for device in to:
        pl.semaphore_signal(barrier, inc=1, device_id=(rep, device), device_id_type=MESH)

    many = range(len(units))
    adds = [(d, u, j) for u in many for j in range(half) for d in (RIGHT, LEFT)]
    steps = [(u, q) for u in many for q in range(each)]

    def own_load(k):
        d, u, j = adds[k]
        return pltpu.make_async_copy(piece(grads, u, to[d], halves[d][j]), own_b.at[k % 2], own_sem.at[k % 2])

    def loads(k):
        u, q = steps[k]
        s = k % 2
        i, layer = units[u]
        return [
            pltpu.make_async_copy(src, dst.at[s], in_sem.at[a, s])
            for a, (src, dst) in enumerate(
                (
                    (piece(grads, u, me, q), g_b),
                    (piece(weights, u, me, q), w_b),
                    (lay[i].of(ms[i], layer, 0, q), m_b),
                    (lay[i].of(vs[i], layer, 0, q), v_b),
                )
            )
        ]

    def store_new(k):
        u, q = steps[k]
        return pltpu.make_async_copy(new_b.at[k % 2], piece(gathered, u, me, q), out_sem.at[0, k % 2])

    def store_sum(k):
        u, q = steps[k]
        i, layer = units[u]
        return pltpu.make_async_copy(sum_b.at[k % 2], lay[i].of(sums[i], layer, 0, q), out_sem.at[1, k % 2])

    own_load(0).start()
    for copy in loads(0):
        copy.start()

    pl.semaphore_wait(barrier, 2)
    for u in many:
        for j in range(half):
            for d in (RIGHT, LEFT):
                first(d, u, j).start()
    for u in many:
        for j in range(half):
            for d in (RIGHT, LEFT):
                plain(d, u, j).start()

    for k, (d, u, j) in enumerate(adds):
        if k + 1 < len(adds):
            own_load(k + 1).start()
        own_load(k).wait()
        first(d, u, j).wait_recv()

        @pl.loop(0, ROWS // STRIP)
        def _(t, d=d, u=u, j=j, k=k):
            at = pl.ds(pl.multiple_of(t * STRIP, STRIP), STRIP)
            mine = own_b[k % 2, at, :].astype(jnp.float32)
            hop[d, u * half + j, at, :] = (hop[d, u * half + j, at, :].astype(jnp.float32) + mine).astype(jnp.bfloat16)

        added(d, u, j).start()

    def send_out(k):
        u, q = steps[k]
        store_new(k).wait()
        for d in (RIGHT, LEFT):
            out(d, u, q).start()

    for k, (u, q) in enumerate(steps):
        s = k % 2
        if k + 1 < len(steps):
            for copy in loads(k + 1):
                copy.start()
        for copy in loads(k):
            copy.wait()
        for d in (RIGHT, LEFT):
            plain(d, u, q % half).wait_recv() if q in halves[1 - d] else added(d, u, q % half).wait_recv()
        if k >= 2:
            store_sum(k - 2).wait()

        @pl.loop(0, ROWS // STRIP)
        def _(t, s=s, k=k):
            at = pl.ds(pl.multiple_of(t * STRIP, STRIP), STRIP)
            g = g_b[s, at, :].astype(jnp.float32) + got[RIGHT, k, at, :].astype(jnp.float32)
            g = (g + got[LEFT, k, at, :].astype(jnp.float32)).astype(jnp.bfloat16)
            sum_b[s, at, :] = g
            new_b[s, at, :] = adamw(w_b[s, at, :].astype(jnp.float32), m_b[s, at, :], v_b[s, at, :], g.astype(jnp.float32))[0]

        store_new(k).start()
        store_sum(k).start()
        if k >= 1:
            send_out(k - 1)
    last = len(steps) - 1
    send_out(last)
    store_sum(last - 1).wait()
    store_sum(last).wait()

    k = 0
    for u in range(LATER):
        for j in range(half):
            for d in (RIGHT, LEFT):
                out(d, u, halves[d][j]).wait_recv()
                bounce = own_b.at[k % 2]
                take = pltpu.make_async_copy(piece(gathered, u, came[d], halves[d][j]), bounce, own_sem.at[k % 2])
                take.start()
                take.wait()
                put = pltpu.make_async_copy(bounce, onward[d].at[u * half + j], own_sem.at[k % 2])
                put.start()
                put.wait()
                k += 1
    for u in many[LATER:]:
        for j in range(half):
            for d in (RIGHT, LEFT):
                out(d, u, halves[d][j]).wait_recv()
                on(d, u, j).start()

    for d in (RIGHT, LEFT):
        for u in many:
            for j in range(half):
                first(d, u, j).wait_send()
                plain(d, u, j).wait_send()
                added(d, u, j).wait_send()
                out(d, u, halves[1 - d][j]).wait_recv()
                if u >= LATER:
                    on(d, u, j).wait()
            for q in range(each):
                out(d, u, q).wait_send()


def spread(lay, *refs):
    brought, wholes = refs[:2], refs[2:5]
    outs, buf, in_sem, out_sem = refs[5:8], refs[8], refs[9], refs[10]
    del wholes
    n = lax.axis_size("dp")
    across = lax.rem(lax.axis_index("dp") + 2, n)
    units = [(i, layer) for i in range(3) for layer in range(lay[i].layers)]
    each = lay[0].each
    half = each // 2
    copies = []
    for d in (RIGHT, LEFT):
        for u in range(LATER):
            for j in range(half):
                i, layer = units[u]
                q = j + d * half
                k = len(copies)
                copies.append(
                    (
                        pltpu.make_async_copy(brought[d].at[u * half + j], buf.at[k], in_sem.at[k]),
                        pltpu.make_async_copy(buf.at[k], lay[i].of(outs[i], layer, across, q), out_sem.at[k]),
                    )
                )
    for take, _ in copies:
        take.start()
    for take, put in copies:
        take.wait()
        put.start()
    for _, put in copies:
        put.wait()


def settle(src, dst):
    dst[...] = src[...]


def settled(x):
    layers, rows, cols = x.shape
    step = (1 << 20) // cols
    spec = pl.BlockSpec((1, step, cols), lambda i, j: (i, j, 0))
    return pl.pallas_call(
        settle,
        grid=(layers, rows // step),
        in_specs=[spec],
        out_specs=spec,
        out_shape=jax.ShapeDtypeStruct(x.shape, x.dtype),
        cost_estimate=pl.CostEstimate(flops=x.size * 40, bytes_accessed=4 * x.size, transcendentals=0),
        name="settle",
    )(x)


def solution(mesh):
    def step(*arrays):
        terms, weights, m, v = (arrays[i : i + 3] for i in (0, 3, 6, 9))
        lay = [Pieces(one.shape) for one in m]
        each = lay[0].each
        assert all(one.each == each for one in lay) and mesh.shape["dp"] == 4
        units = sum(one.layers for one in lay)
        half = each // 2
        anywhere = pl.BlockSpec(memory_space=pl.ANY)
        bf16 = jnp.bfloat16
        dma = pltpu.SemaphoreType.DMA
        res = pl.pallas_call(
            functools.partial(kernel, lay),
            out_shape=[jax.ShapeDtypeStruct(one.shape, bf16) for one in m]
            + [jax.ShapeDtypeStruct(one.shape, bf16) for one in weights]
            + [jax.ShapeDtypeStruct((LATER * half, ROWS, COLS), bf16)] * 2,
            in_specs=[anywhere] * 12,
            out_specs=[anywhere] * 8,
            scratch_shapes=[
                pltpu.VMEM((2, units * half, ROWS, COLS), bf16),
                pltpu.VMEM((2, units * each, ROWS, COLS), bf16),
                pltpu.VMEM((2, ROWS, COLS), bf16),
                pltpu.VMEM((2, ROWS, COLS), bf16),
                pltpu.VMEM((2, ROWS, COLS), bf16),
                pltpu.VMEM((2, ROWS, COLS), jnp.float32),
                pltpu.VMEM((2, ROWS, COLS), jnp.float32),
                pltpu.VMEM((2, ROWS, COLS), bf16),
                pltpu.VMEM((2, ROWS, COLS), bf16),
                dma((2, units * half)), dma((2, units * half)),
                dma((2, units * each)), dma((2, units * each)),
                dma((2, units * each)), dma((2, units * each)),
                dma((2, units * half)), dma((2, units * half)),
                dma((2,)), dma((4, 2)), dma((2, 2)),
            ],
            compiler_params=pltpu.CompilerParams(collective_id=0, has_side_effects=True, vmem_limit_bytes=VMEM_LIMIT),
            name="sum_step_gather",
        )(*(t[0] for t in terms), *weights, *m, *v)
        sums, gathered, onward = res[:3], res[3:6], res[6:8]
        n = mesh.shape["dp"]
        brought = [
            lax.ppermute(onward[RIGHT], "dp", [(i, (i + 1) % n) for i in range(n)]),
            lax.ppermute(onward[LEFT], "dp", [(i, (i - 1) % n) for i in range(n)]),
        ]
        wholes = [settled(one) for one in gathered]
        new_m, new_v = [], []
        for one_m, one_v, g in zip(m, v, sums, strict=True):
            g = g.astype(jnp.float32)
            new_m.append(0.9 * one_m + 0.1 * g)
            new_v.append(0.95 * one_v + 0.05 * g * g)
        pieces = 2 * LATER * half
        wholes = pl.pallas_call(
            functools.partial(spread, lay),
            out_shape=[jax.ShapeDtypeStruct(one.shape, one.dtype) for one in wholes],
            in_specs=[anywhere] * 5,
            out_specs=[anywhere] * 3,
            input_output_aliases={2: 0, 3: 1, 4: 2},
            scratch_shapes=[pltpu.VMEM((pieces, ROWS, COLS), bf16), dma((pieces,)), dma((pieces,))],
            name="spread",
        )(*brought, *wholes)
        return (*wholes, *new_m, *new_v)

    all_of, cut = P(None, None, None), P(None, "dp", None)
    return jax.shard_map(
        step,
        mesh=mesh,
        in_specs=(P(("rep", "dp"), None, None, None),) * 3 + (all_of,) * 3 + (cut,) * 6,
        out_specs=(P("rep", None, None),) * 3 + (P("rep", "dp", None),) * 6,
        check_vma=False,
    )
```

```python
import functools

import jax
import jax.numpy as jnp
from jax import lax
from jax.experimental import pallas as pl
from jax.experimental.pallas import tpu as pltpu
from jax.sharding import PartitionSpec as P


MESH = pl.DeviceIdType.MESH
ROWS, COLS = 256, 1024
RIGHT, LEFT = 0, 1
STRIP = 32
LATER = 4
LAST = 1
VMEM_LIMIT = 67043328


def adamw(w, m, v, g):
    m = 0.9 * m + 0.1 * g
    v = 0.95 * v + 0.05 * g * g
    step = m * lax.rsqrt(v + 1e-8) + 0.1 * w
    return (w - 0.02 * step).astype(jnp.bfloat16), m, v


class Pieces:
    def __init__(self, block):
        self.layers, self.rows, cols = block
        self.across = cols // COLS
        self.each = (self.rows // ROWS) * self.across
        assert self.rows % ROWS == 0 and cols % COLS == 0 and self.each % 2 == 0

    def of(self, ref, layer, owner, q):
        start = pl.multiple_of(owner * self.rows + (q // self.across) * ROWS, ROWS)
        return ref.at[layer, pl.ds(start, ROWS), pl.ds((q % self.across) * COLS, COLS)]


def kernel(lay, *refs):
    grads, weights, ms, vs, sums, gathered = (refs[i : i + 3] for i in range(0, 18, 3))
    onward = refs[18:22]
    (
        hop, got, own_b, g_b, w_b, m_b, v_b, sum_b, new_b,
        s1_send, s1_recv, s2_send, s2_recv, a1_send, a1_recv, a2_send, a2_recv,
        own_sem, in_sem, out_sem,
    ) = refs[22:]
    n = lax.axis_size("dp")
    me = lax.axis_index("dp")
    rep = lax.axis_index("rep")
    right, left, across = lax.rem(me + 1, n), lax.rem(me + n - 1, n), lax.rem(me + 2, n)
    to = (right, left)
    came = (left, right)

    units = [(i, layer) for i in range(3) for layer in range(lay[i].layers)]
    each = lay[0].each
    half = each // 2
    halves = (range(0, half), range(half, each))

    def remote(src, dst, sends, recvs, d, k):
        return pltpu.make_async_remote_copy(
            src_ref=src,
            dst_ref=dst,
            send_sem=sends.at[d, k],
            recv_sem=recvs.at[d, k],
            device_id=(rep, to[d]),
            device_id_type=MESH,
        )

    def piece(arrays, u, owner, q):
        i, layer = units[u]
        return lay[i].of(arrays[i], layer, owner, q)

    def first(d, u, j):
        return remote(piece(grads, u, across, halves[d][j]), hop.at[d, u * half + j], s1_send, s1_recv, d, u * half + j)

    def plain(d, u, j):
        q = halves[1 - d][j]
        return remote(piece(grads, u, to[d], q), got.at[d, u * each + q], s2_send, s2_recv, d, u * each + q)

    def added(d, u, j):
        q = halves[d][j]
        return remote(hop.at[d, u * half + j], got.at[d, u * each + q], s2_send, s2_recv, d, u * each + q)

    def out(d, u, q):
        src = piece(gathered, u, me, q)
        return remote(src, src, a1_send, a1_recv, d, u * each + q)

    def on(d, u, j):
        src = piece(gathered, u, came[d], halves[d][j])
        return remote(src, src, a2_send, a2_recv, d, u * half + j)

    barrier = pltpu.get_barrier_semaphore()
    for device in to:
        pl.semaphore_signal(barrier, inc=1, device_id=(rep, device), device_id_type=MESH)

    many = range(len(units))
    adds = [(d, u, j) for u in many for j in range(half) for d in (RIGHT, LEFT)]
    steps = [(u, q) for u in many for q in range(each)]

    def own_load(k):
        d, u, j = adds[k]
        return pltpu.make_async_copy(piece(grads, u, to[d], halves[d][j]), own_b.at[k % 2], own_sem.at[k % 2])

    def loads(k):
        u, q = steps[k]
        s = k % 2
        i, layer = units[u]
        return [
            pltpu.make_async_copy(src, dst.at[s], in_sem.at[a, s])
            for a, (src, dst) in enumerate(
                (
                    (piece(grads, u, me, q), g_b),
                    (piece(weights, u, me, q), w_b),
                    (lay[i].of(ms[i], layer, 0, q), m_b),
                    (lay[i].of(vs[i], layer, 0, q), v_b),
                )
            )
        ]

    def store_new(k):
        u, q = steps[k]
        return pltpu.make_async_copy(new_b.at[k % 2], piece(gathered, u, me, q), out_sem.at[0, k % 2])

    def store_sum(k):
        u, q = steps[k]
        i, layer = units[u]
        return pltpu.make_async_copy(sum_b.at[k % 2], lay[i].of(sums[i], layer, 0, q), out_sem.at[1, k % 2])

    own_load(0).start()
    for copy in loads(0):
        copy.start()

    pl.semaphore_wait(barrier, 2)
    for u in many:
        for j in range(half):
            for d in (RIGHT, LEFT):
                first(d, u, j).start()
    for u in many:
        for j in range(half):
            for d in (RIGHT, LEFT):
                plain(d, u, j).start()

    for k, (d, u, j) in enumerate(adds):
        if k + 1 < len(adds):
            own_load(k + 1).start()
        own_load(k).wait()
        first(d, u, j).wait_recv()

        @pl.loop(0, ROWS // STRIP)
        def _(t, d=d, u=u, j=j, k=k):
            at = pl.ds(pl.multiple_of(t * STRIP, STRIP), STRIP)
            mine = own_b[k % 2, at, :].astype(jnp.float32)
            hop[d, u * half + j, at, :] = (hop[d, u * half + j, at, :].astype(jnp.float32) + mine).astype(jnp.bfloat16)

        added(d, u, j).start()

    def send_out(k):
        u, q = steps[k]
        store_new(k).wait()
        for d in (RIGHT, LEFT):
            out(d, u, q).start()

    for k, (u, q) in enumerate(steps):
        s = k % 2
        if k + 1 < len(steps):
            for copy in loads(k + 1):
                copy.start()
        for copy in loads(k):
            copy.wait()
        for d in (RIGHT, LEFT):
            plain(d, u, q % half).wait_recv() if q in halves[1 - d] else added(d, u, q % half).wait_recv()
        if k >= 2:
            store_sum(k - 2).wait()

        @pl.loop(0, ROWS // STRIP)
        def _(t, s=s, k=k):
            at = pl.ds(pl.multiple_of(t * STRIP, STRIP), STRIP)
            g = g_b[s, at, :].astype(jnp.float32) + got[RIGHT, k, at, :].astype(jnp.float32)
            g = (g + got[LEFT, k, at, :].astype(jnp.float32)).astype(jnp.bfloat16)
            sum_b[s, at, :] = g
            new_b[s, at, :] = adamw(w_b[s, at, :].astype(jnp.float32), m_b[s, at, :], v_b[s, at, :], g.astype(jnp.float32))[0]

        store_new(k).start()
        store_sum(k).start()
        if k >= 1:
            send_out(k - 1)
    last = len(steps) - 1
    send_out(last)
    store_sum(last - 1).wait()
    store_sum(last).wait()

    split = LATER * half - LAST
    for u in range(LATER):
        for j in range(half):
            for d in (RIGHT, LEFT):
                k = u * half + j
                out(d, u, halves[d][j]).wait_recv()
                take = pltpu.make_async_copy(piece(gathered, u, came[d], halves[d][j]), own_b.at[d], own_sem.at[d])
                take.start()
                take.wait()
                dst = onward[d].at[k] if k < split else onward[2 + d].at[k - split]
                put = pltpu.make_async_copy(own_b.at[d], dst, own_sem.at[d])
                put.start()
                put.wait()
    for u in many[LATER:]:
        for j in range(half):
            for d in (RIGHT, LEFT):
                out(d, u, halves[d][j]).wait_recv()
                on(d, u, j).start()

    for d in (RIGHT, LEFT):
        for u in many:
            for j in range(half):
                first(d, u, j).wait_send()
                plain(d, u, j).wait_send()
                added(d, u, j).wait_send()
                out(d, u, halves[1 - d][j]).wait_recv()
                if u >= LATER:
                    on(d, u, j).wait()
            for q in range(each):
                out(d, u, q).wait_send()


def spread(lay, first, *refs):
    brought, outs, sem = refs[:2], refs[5:8], refs[8]
    n = lax.axis_size("dp")
    across = lax.rem(lax.axis_index("dp") + 2, n)
    units = [(i, layer) for i in range(3) for layer in range(lay[i].layers)]
    half = lay[0].each // 2
    copies = []
    for d in (RIGHT, LEFT):
        for k in range(brought[d].shape[0]):
            i, layer = units[(first + k) // half]
            q = (first + k) % half + d * half
            copies.append(pltpu.make_async_copy(brought[d].at[k], lay[i].of(outs[i], layer, across, q), sem.at[len(copies)]))
    for copy in copies:
        copy.start()
    for copy in copies:
        copy.wait()


def settle(src, dst):
    dst[...] = src[...]


def settled(x):
    layers, rows, cols = x.shape
    step = (1 << 20) // cols
    spec = pl.BlockSpec((1, step, cols), lambda i, j: (i, j, 0))
    return pl.pallas_call(
        settle,
        grid=(layers, rows // step),
        in_specs=[spec],
        out_specs=spec,
        out_shape=jax.ShapeDtypeStruct(x.shape, x.dtype),
        cost_estimate=pl.CostEstimate(flops=x.size * 40, bytes_accessed=4 * x.size, transcendentals=0),
        name="settle",
    )(x)


def solution(mesh):
    def step(*arrays):
        terms, weights, m, v = (arrays[i : i + 3] for i in (0, 3, 6, 9))
        lay = [Pieces(one.shape) for one in m]
        each = lay[0].each
        assert all(one.each == each for one in lay) and mesh.shape["dp"] == 4
        units = sum(one.layers for one in lay)
        half = each // 2
        anywhere = pl.BlockSpec(memory_space=pl.ANY)
        bf16 = jnp.bfloat16
        dma = pltpu.SemaphoreType.DMA
        res = pl.pallas_call(
            functools.partial(kernel, lay),
            out_shape=[jax.ShapeDtypeStruct(one.shape, bf16) for one in m]
            + [jax.ShapeDtypeStruct(one.shape, bf16) for one in weights]
            + [jax.ShapeDtypeStruct((LATER * half - LAST, ROWS, COLS), bf16)] * 2
            + [jax.ShapeDtypeStruct((LAST, ROWS, COLS), bf16)] * 2,
            in_specs=[anywhere] * 12,
            out_specs=[anywhere] * 10,
            scratch_shapes=[
                pltpu.VMEM((2, units * half, ROWS, COLS), bf16),
                pltpu.VMEM((2, units * each, ROWS, COLS), bf16),
                pltpu.VMEM((2, ROWS, COLS), bf16),
                pltpu.VMEM((2, ROWS, COLS), bf16),
                pltpu.VMEM((2, ROWS, COLS), bf16),
                pltpu.VMEM((2, ROWS, COLS), jnp.float32),
                pltpu.VMEM((2, ROWS, COLS), jnp.float32),
                pltpu.VMEM((2, ROWS, COLS), bf16),
                pltpu.VMEM((2, ROWS, COLS), bf16),
                dma((2, units * half)), dma((2, units * half)),
                dma((2, units * each)), dma((2, units * each)),
                dma((2, units * each)), dma((2, units * each)),
                dma((2, units * half)), dma((2, units * half)),
                dma((2,)), dma((4, 2)), dma((2, 2)),
            ],
            compiler_params=pltpu.CompilerParams(collective_id=0, has_side_effects=True, vmem_limit_bytes=VMEM_LIMIT),
            name="sum_step_gather",
        )(*(t[0] for t in terms), *weights, *m, *v)
        sums, gathered, onward = res[:3], res[3:6], res[6:10]
        n = mesh.shape["dp"]
        brought = []
        for k in (0, 2):
            for x, hop in zip(onward[k : k + 2], (1, -1), strict=True):
                brought.append(lax.ppermute(x, "dp", [(i, (i + hop) % n) for i in range(n)]))
        wholes = [settled(one) for one in gathered]
        new_m, new_v = [], []
        for one_m, one_v, g in zip(m, v, sums, strict=True):
            g = g.astype(jnp.float32)
            new_m.append(0.9 * one_m + 0.1 * g)
            new_v.append(0.95 * one_v + 0.05 * g * g)
        for pair, first in ((brought[:2], 0), (brought[2:], LATER * half - LAST)):
            wholes = pl.pallas_call(
                functools.partial(spread, lay, first),
                out_shape=[jax.ShapeDtypeStruct(one.shape, one.dtype) for one in wholes],
                in_specs=[pl.BlockSpec(memory_space=pltpu.VMEM)] * 2 + [anywhere] * 3,
                out_specs=[anywhere] * 3,
                input_output_aliases={2: 0, 3: 1, 4: 2},
                scratch_shapes=[dma((2 * pair[0].shape[0],))],
                compiler_params=pltpu.CompilerParams(vmem_limit_bytes=24 << 20),
                name="spread",
            )(*pair, *wholes)
        return (*wholes, *new_m, *new_v)

    all_of, cut = P(None, None, None), P(None, "dp", None)
    return jax.shard_map(
        step,
        mesh=mesh,
        in_specs=(P(("rep", "dp"), None, None, None),) * 3 + (all_of,) * 3 + (cut,) * 6,
        out_specs=(P("rep", None, None),) * 3 + (P("rep", "dp", None),) * 6,
        check_vma=False,
    )
```

```python
import functools

import jax
import jax.numpy as jnp
from jax import lax
from jax.experimental import pallas as pl
from jax.experimental.pallas import tpu as pltpu
from jax.sharding import PartitionSpec as P


MESH = pl.DeviceIdType.MESH
ROWS, COLS = 256, 1024
RIGHT, LEFT = 0, 1
STRIP = 32
LATER = 4
LAST = 1
PAUSE = 10
FLIGHT = 32
VMEM_LIMIT = 67043328


def adamw(w, m, v, g):
    m = 0.9 * m + 0.1 * g
    v = 0.95 * v + 0.05 * g * g
    step = m * lax.rsqrt(v + 1e-8) + 0.1 * w
    return (w - 0.02 * step).astype(jnp.bfloat16), m, v


class Lay:
    def __init__(self, block):
        self.layers, self.rows, self.cols = block
        self.across = self.cols // COLS
        tiles = (self.rows // ROWS) * self.across
        assert self.rows % ROWS == 0 and self.cols % COLS == 0 and tiles % 2 == 0
        assert self.across == 1 or self.rows == ROWS
        self.tiles = tiles // 2
        self.half = (self.rows // 2, self.cols) if self.across == 1 else (self.rows, self.cols // 2)

    def of(self, ref, layer, owner, h):
        down, over = (h, 0) if self.across == 1 else (0, h)
        start = pl.multiple_of(owner * self.rows + down * self.half[0], ROWS)
        return ref.at[layer, pl.ds(start, self.half[0]), pl.ds(over * self.half[1], self.half[1])]

    def tile(self, ref, layer, owner, h, t):
        q = h * self.tiles + t
        start = pl.multiple_of(owner * self.rows + (q // self.across) * ROWS, ROWS)
        return ref.at[layer, pl.ds(start, ROWS), pl.ds((q % self.across) * COLS, COLS)]

    def inside(self, t, strip):
        down, over = (t, 0) if self.across == 1 else (0, t)
        return pl.ds(pl.multiple_of(down * ROWS + strip * STRIP, STRIP), STRIP), pl.ds(over * COLS, COLS)


def kernel(lay, *refs):
    grads, weights, ms, vs, sums, gathered = (refs[i : i + 3] for i in range(0, 18, 3))
    onward, hop, got = refs[18:22], refs[22:25], refs[25:28]
    (
        own_b, g_b, w_b, m_b, v_b, sum_b, new_b,
        s1_send, s1_recv, s2_send, s2_recv, a1_send, a1_recv, a2_send, a2_recv,
        own_sem, in_sem, out_sem,
    ) = refs[28:]
    n = lax.axis_size("dp")
    me = lax.axis_index("dp")
    rep = lax.axis_index("rep")
    right, left, across = lax.rem(me + 1, n), lax.rem(me + n - 1, n), lax.rem(me + 2, n)
    to = (right, left)
    came = (left, right)
    units = [(i, layer) for i in range(3) for layer in range(lay[i].layers)]
    many = range(len(units))
    tiles = lay[0].tiles
    ways = (RIGHT, LEFT)

    def remote(src, dst, sends, recvs, d, k):
        return pltpu.make_async_remote_copy(
            src_ref=src,
            dst_ref=dst,
            send_sem=sends.at[d, k],
            recv_sem=recvs.at[d, k],
            device_id=(rep, to[d]),
            device_id_type=MESH,
        )

    def part(arrays, u, owner, h):
        i, layer = units[u]
        return lay[i].of(arrays[i], layer, owner, h)

    def tile(arrays, u, owner, h, t):
        i, layer = units[u]
        return lay[i].tile(arrays[i], layer, owner, h, t)

    def first(d, u):
        i, layer = units[u]
        return remote(part(grads, u, across, d), hop[i].at[d, layer], s1_send, s1_recv, d, u)

    def plain(d, u):
        i, layer = units[u]
        return remote(part(grads, u, to[d], 1 - d), got[i].at[d, layer, 1 - d], s2_send, s2_recv, d, 2 * u + 1 - d)

    def added(d, u):
        i, layer = units[u]
        return remote(hop[i].at[d, layer], got[i].at[d, layer, d], s2_send, s2_recv, d, 2 * u + d)

    def out(d, u, h):
        src = part(gathered, u, me, h)
        return remote(src, src, a1_send, a1_recv, d, 2 * u + h)

    def on(d, u):
        src = part(gathered, u, came[d], d)
        return remote(src, src, a2_send, a2_recv, d, u)

    barrier = pltpu.get_barrier_semaphore()
    for device in to:
        pl.semaphore_signal(barrier, inc=1, device_id=(rep, device), device_id_type=MESH)

    adds = [(d, u, t) for u in many for d in ways for t in range(tiles)]
    steps = [(u, h, t) for u in many for h in range(2) for t in range(tiles)]

    def own_load(k):
        d, u, t = adds[k]
        return pltpu.make_async_copy(tile(grads, u, to[d], d, t), own_b.at[k % 2], own_sem.at[k % 2])

    def loads(k):
        u, h, t = steps[k]
        s = k % 2
        pairs = ((tile(grads, u, me, h, t), g_b), (tile(weights, u, me, h, t), w_b), (tile(ms, u, 0, h, t), m_b), (tile(vs, u, 0, h, t), v_b))
        return [pltpu.make_async_copy(src, dst.at[s], in_sem.at[a, s]) for a, (src, dst) in enumerate(pairs)]

    def store_new(k):
        u, h, t = steps[k]
        return pltpu.make_async_copy(new_b.at[k % 2], tile(gathered, u, me, h, t), out_sem.at[0, k % 2])

    def store_sum(k):
        u, h, t = steps[k]
        return pltpu.make_async_copy(sum_b.at[k % 2], tile(sums, u, 0, h, t), out_sem.at[1, k % 2])

    own_load(0).start()
    for copy in loads(0):
        copy.start()

    pl.semaphore_wait(barrier, 2)

    @pl.when(lax.rem(rep, 2) == 1)
    def _():
        @pl.loop(0, PAUSE)
        def _(_):
            pause = pltpu.make_async_copy(tile(weights, 0, me, 0, 0), new_b.at[0], own_sem.at[1])
            pause.start()
            pause.wait()

    for u in many:
        for d in ways:
            first(d, u).start()
    for u in many:
        for d in ways:
            plain(d, u).start()

    for k, (d, u, t) in enumerate(adds):
        i, layer = units[u]
        if k + 1 < len(adds):
            own_load(k + 1).start()
        own_load(k).wait()
        if t == 0:
            first(d, u).wait_recv()

        @pl.loop(0, ROWS // STRIP)
        def _(strip, d=d, i=i, layer=layer, t=t, k=k):
            at = pl.ds(pl.multiple_of(strip * STRIP, STRIP), STRIP)
            there = (d, layer, *lay[i].inside(t, strip))
            hop[i][there] = (hop[i][there].astype(jnp.float32) + own_b[k % 2, at, :].astype(jnp.float32)).astype(jnp.bfloat16)

        if t == tiles - 1:
            added(d, u).start()

    def send_out(k):
        u, h, t = steps[k]
        store_new(k).wait()
        if t == tiles - 1:
            for d in ways:
                out(d, u, h).start()

    for k, (u, h, t) in enumerate(steps):
        s = k % 2
        i, layer = units[u]
        if k + 1 < len(steps):
            for copy in loads(k + 1):
                copy.start()
        for copy in loads(k):
            copy.wait()
        if t == 0:
            for d in ways:
                (added if d == h else plain)(d, u).wait_recv()
        if k >= 2:
            store_sum(k - 2).wait()

        @pl.loop(0, ROWS // STRIP)
        def _(strip, s=s, i=i, layer=layer, h=h, t=t):
            at = pl.ds(pl.multiple_of(strip * STRIP, STRIP), STRIP)
            there = (layer, h, *lay[i].inside(t, strip))
            g = g_b[s, at, :].astype(jnp.float32) + got[i][(RIGHT, *there)].astype(jnp.float32)
            g = (g + got[i][(LEFT, *there)].astype(jnp.float32)).astype(jnp.bfloat16)
            sum_b[s, at, :] = g
            new_b[s, at, :] = adamw(w_b[s, at, :].astype(jnp.float32), m_b[s, at, :], v_b[s, at, :], g.astype(jnp.float32))[0]

        store_new(k).start()
        store_sum(k).start()
        if k >= 1:
            send_out(k - 1)
    end = len(steps) - 1
    send_out(end)
    store_sum(end - 1).wait()
    store_sum(end).wait()

    split = LATER * tiles - LAST
    for u in range(LATER):
        for d in ways:
            out(d, u, d).wait_recv()
            for t in range(tiles):
                k = u * tiles + t
                take = pltpu.make_async_copy(tile(gathered, u, came[d], d, t), own_b.at[d], own_sem.at[d])
                take.start()
                take.wait()
                dst = onward[d].at[k] if k < split else onward[2 + d].at[k - split]
                put = pltpu.make_async_copy(own_b.at[d], dst, own_sem.at[d])
                put.start()
                put.wait()
    for u in many[LATER:]:
        for d in ways:
            out(d, u, d).wait_recv()
            on(d, u).start()

    for u in many:
        for d in ways:
            first(d, u).wait_send()
            plain(d, u).wait_send()
            added(d, u).wait_send()
            out(d, u, 1 - d).wait_recv()
            for h in range(2):
                out(d, u, h).wait_send()
            if u >= LATER:
                on(d, u).wait()


def settle(lay, *refs):
    ins, outs, buf, in_sem, out_sem = refs[:3], refs[3:6], refs[6], refs[7], refs[8]
    n = lax.axis_size("dp")
    me = lax.axis_index("dp")
    units = [(i, layer) for i in range(3) for layer in range(lay[i].layers)]
    tiles = [
        (i, layer, lax.rem(me + hops, n), h, t)
        for u, (i, layer) in enumerate(units)
        for hops in range(4)
        for h in range(2)
        for t in range(lay[i].tiles)
        if hops != 2 or u >= LATER
    ]

    def take(k):
        i, *where = tiles[k]
        return pltpu.make_async_copy(lay[i].tile(ins[i], *where), buf.at[k % FLIGHT], in_sem.at[k % FLIGHT])

    def put(k):
        i, *where = tiles[k]
        return pltpu.make_async_copy(buf.at[k % FLIGHT], lay[i].tile(outs[i], *where), out_sem.at[k % FLIGHT])

    lag = FLIGHT // 2
    for k in range(len(tiles) + lag):
        if k < len(tiles):
            if k >= FLIGHT:
                put(k - FLIGHT).wait()
            take(k).start()
        if k >= lag:
            take(k - lag).wait()
            put(k - lag).start()
    for k in range(len(tiles) - FLIGHT, len(tiles)):
        put(k).wait()


def spread(lay, first, *refs):
    brought, outs, sem = refs[:2], refs[5:8], refs[8]
    n = lax.axis_size("dp")
    across = lax.rem(lax.axis_index("dp") + 2, n)
    units = [(i, layer) for i in range(3) for layer in range(lay[i].layers)]
    tiles = lay[0].tiles
    copies = []
    for d in (RIGHT, LEFT):
        for k in range(brought[d].shape[0]):
            i, layer = units[(first + k) // tiles]
            dst = lay[i].tile(outs[i], layer, across, d, (first + k) % tiles)
            copies.append(pltpu.make_async_copy(brought[d].at[k], dst, sem.at[len(copies)]))
    for copy in copies:
        copy.start()
    for copy in copies:
        copy.wait()


def solution(mesh):
    def step(*arrays):
        terms, weights, m, v = (arrays[i : i + 3] for i in (0, 3, 6, 9))
        lay = [Lay(one.shape) for one in m]
        tiles = lay[0].tiles
        assert all(one.tiles == tiles for one in lay) and mesh.shape["dp"] == 4
        units = sum(one.layers for one in lay)
        anywhere = pl.BlockSpec(memory_space=pl.ANY)
        bf16 = jnp.bfloat16
        dma = pltpu.SemaphoreType.DMA
        res = pl.pallas_call(
            functools.partial(kernel, lay),
            out_shape=[jax.ShapeDtypeStruct(one.shape, bf16) for one in m]
            + [jax.ShapeDtypeStruct(one.shape, bf16) for one in weights]
            + [jax.ShapeDtypeStruct((LATER * tiles - LAST, ROWS, COLS), bf16)] * 2
            + [jax.ShapeDtypeStruct((LAST, ROWS, COLS), bf16)] * 2,
            in_specs=[anywhere] * 12,
            out_specs=[anywhere] * 10,
            scratch_shapes=[
                *(pltpu.VMEM((2, one.layers, *one.half), bf16) for one in lay),
                *(pltpu.VMEM((2, one.layers, 2, *one.half), bf16) for one in lay),
                pltpu.VMEM((2, ROWS, COLS), bf16),
                pltpu.VMEM((2, ROWS, COLS), bf16),
                pltpu.VMEM((2, ROWS, COLS), bf16),
                pltpu.VMEM((2, ROWS, COLS), jnp.float32),
                pltpu.VMEM((2, ROWS, COLS), jnp.float32),
                pltpu.VMEM((2, ROWS, COLS), bf16),
                pltpu.VMEM((2, ROWS, COLS), bf16),
                dma((2, units)), dma((2, units)),
                dma((2, 2 * units)), dma((2, 2 * units)),
                dma((2, 2 * units)), dma((2, 2 * units)),
                dma((2, units)), dma((2, units)),
                dma((2,)), dma((4, 2)), dma((2, 2)),
            ],
            compiler_params=pltpu.CompilerParams(collective_id=0, has_side_effects=True, vmem_limit_bytes=VMEM_LIMIT),
            name="sum_step_gather",
        )(*(t[0] for t in terms), *weights, *m, *v)
        sums, gathered, onward = res[:3], res[3:6], res[6:10]
        n = mesh.shape["dp"]
        brought = []
        for k in (0, 2):
            for x, hop in zip(onward[k : k + 2], (1, -1), strict=True):
                brought.append(lax.ppermute(x, "dp", [(i, (i + hop) % n) for i in range(n)]))
        size = sum(one.size for one in gathered)
        wholes = pl.pallas_call(
            functools.partial(settle, lay),
            out_shape=[jax.ShapeDtypeStruct(one.shape, one.dtype) for one in gathered],
            in_specs=[anywhere] * 3,
            out_specs=[anywhere] * 3,
            scratch_shapes=[pltpu.VMEM((FLIGHT, ROWS, COLS), bf16), dma((FLIGHT,)), dma((FLIGHT,))],
            compiler_params=pltpu.CompilerParams(vmem_limit_bytes=54 << 20),
            cost_estimate=pl.CostEstimate(flops=size * 40, bytes_accessed=4 * size, transcendentals=0),
            name="settle",
        )(*gathered)
        new_m, new_v = [], []
        for one_m, one_v, g in zip(m, v, sums, strict=True):
            g = g.astype(jnp.float32)
            new_m.append(0.9 * one_m + 0.1 * g)
            new_v.append(0.95 * one_v + 0.05 * g * g)
        for pair, first in ((brought[:2], 0), (brought[2:], LATER * tiles - LAST)):
            wholes = pl.pallas_call(
                functools.partial(spread, lay, first),
                out_shape=[jax.ShapeDtypeStruct(one.shape, one.dtype) for one in wholes],
                in_specs=[pl.BlockSpec(memory_space=pltpu.VMEM)] * 2 + [anywhere] * 3,
                out_specs=[anywhere] * 3,
                input_output_aliases={2: 0, 3: 1, 4: 2},
                scratch_shapes=[dma((2 * pair[0].shape[0],))],
                compiler_params=pltpu.CompilerParams(vmem_limit_bytes=24 << 20),
                name="spread",
            )(*pair, *wholes)
        return (*wholes, *new_m, *new_v)

    all_of, cut = P(None, None, None), P(None, "dp", None)
    return jax.shard_map(
        step,
        mesh=mesh,
        in_specs=(P(("rep", "dp"), None, None, None),) * 3 + (all_of,) * 3 + (cut,) * 6,
        out_specs=(P("rep", None, None),) * 3 + (P("rep", "dp", None),) * 6,
        check_vma=False,
    )
```

```python
import functools

import jax
import jax.numpy as jnp
from jax import lax
from jax.experimental import pallas as pl
from jax.experimental.pallas import tpu as pltpu
from jax.sharding import PartitionSpec as P


MESH = pl.DeviceIdType.MESH
ROWS, COLS = 256, 1024
RIGHT, LEFT = 0, 1
STRIP = 32
LATER = 4
LAST = 1
PAUSE = 96
FLIGHT = 32
VMEM_LIMIT = 67043328


def adamw(w, m, v, g):
    m = 0.9 * m + 0.1 * g
    v = 0.95 * v + 0.05 * g * g
    step = m * lax.rsqrt(v + 1e-8) + 0.1 * w
    return (w - 0.02 * step).astype(jnp.bfloat16), m, v


class Lay:
    def __init__(self, block):
        self.layers, self.rows, self.cols = block
        self.across = self.cols // COLS
        tiles = (self.rows // ROWS) * self.across
        assert self.rows % ROWS == 0 and self.cols % COLS == 0 and tiles % 2 == 0
        assert self.across == 1 or self.rows == ROWS
        self.tiles = tiles // 2
        self.half = (self.rows // 2, self.cols) if self.across == 1 else (self.rows, self.cols // 2)

    def of(self, ref, layer, owner, h):
        down, over = (h, 0) if self.across == 1 else (0, h)
        start = pl.multiple_of(owner * self.rows + down * self.half[0], ROWS)
        return ref.at[layer, pl.ds(start, self.half[0]), pl.ds(over * self.half[1], self.half[1])]

    def whole(self, ref, layer, owner):
        return ref.at[layer, pl.ds(pl.multiple_of(owner * self.rows, ROWS), self.rows)]

    def tile(self, ref, layer, owner, h, t):
        q = h * self.tiles + t
        start = pl.multiple_of(owner * self.rows + (q // self.across) * ROWS, ROWS)
        return ref.at[layer, pl.ds(start, ROWS), pl.ds((q % self.across) * COLS, COLS)]

    def inside(self, t, strip):
        down, over = (t, 0) if self.across == 1 else (0, t)
        if strip is None:
            return pl.ds(down * ROWS, ROWS), pl.ds(over * COLS, COLS)
        return pl.ds(pl.multiple_of(down * ROWS + strip * STRIP, STRIP), STRIP), pl.ds(over * COLS, COLS)


def kernel(lay, *refs):
    grads, weights, ms, vs, sums, gathered = (refs[i : i + 3] for i in range(0, 18, 3))
    onward, hop, got = refs[18:22], refs[22:25], refs[25:28]
    (
        own_b, g_b, w_b, m_b, v_b, sum_b, new_b,
        s1_send, s1_recv, s2_send, s2_recv, a1_send, a1_recv, a2_send, a2_recv,
        own_sem, in_sem, out_sem, put_sem,
    ) = refs[28:]
    n = lax.axis_size("dp")
    me = lax.axis_index("dp")
    rep = lax.axis_index("rep")
    right, left, across = lax.rem(me + 1, n), lax.rem(me + n - 1, n), lax.rem(me + 2, n)
    to = (right, left)
    came = (left, right)
    units = [(i, layer) for i in range(3) for layer in range(lay[i].layers)]
    many = range(len(units))
    tiles = lay[0].tiles
    ways = (RIGHT, LEFT)

    def remote(src, dst, sends, recvs, d, k):
        return pltpu.make_async_remote_copy(
            src_ref=src,
            dst_ref=dst,
            send_sem=sends.at[d, k],
            recv_sem=recvs.at[d, k],
            device_id=(rep, to[d]),
            device_id_type=MESH,
        )

    def part(arrays, u, owner, h):
        i, layer = units[u]
        return lay[i].of(arrays[i], layer, owner, h)

    def tile(arrays, u, owner, h, t):
        i, layer = units[u]
        return lay[i].tile(arrays[i], layer, owner, h, t)

    def first(d, i):
        return remote(lay[i].of(grads[i], slice(None), across, d), hop[i].at[d], s1_send, s1_recv, d, i)

    def plain(d, i):
        src = lay[i].of(grads[i], slice(None), to[d], 1 - d)
        return remote(src, got[i].at[d, 1 - d], s2_send, s2_recv, d, 2 * i + 1 - d)

    def added(d, i):
        return remote(hop[i].at[d], got[i].at[d, d], s2_send, s2_recv, d, 2 * i + d)

    def out(d, u):
        i, layer = units[u]
        src = lay[i].whole(gathered[i], layer, me)
        return remote(src, src, a1_send, a1_recv, d, u)

    def on(d, u):
        src = part(gathered, u, came[d], d)
        return remote(src, src, a2_send, a2_recv, d, u)

    barrier = pltpu.get_barrier_semaphore()
    for device in to:
        pl.semaphore_signal(barrier, inc=1, device_id=(rep, device), device_id_type=MESH)

    adds = [(d, u, t) for i in range(3) for d in ways for u in many if units[u][0] == i for t in range(tiles)]
    steps = [(u, h, t) for u in many for h in range(2) for t in range(tiles)]

    def own_load(k):
        d, u, t = adds[k]
        return pltpu.make_async_copy(tile(grads, u, to[d], d, t), own_b.at[k % 2], own_sem.at[k % 2])

    def loads(k):
        u, h, t = steps[k]
        s = k % 2
        pairs = ((tile(grads, u, me, h, t), g_b), (tile(weights, u, me, h, t), w_b), (tile(ms, u, 0, h, t), m_b), (tile(vs, u, 0, h, t), v_b))
        return [pltpu.make_async_copy(src, dst.at[s], in_sem.at[a, s]) for a, (src, dst) in enumerate(pairs)]

    def store_new(k):
        u, h, t = steps[k]
        return pltpu.make_async_copy(new_b.at[k % 2], tile(gathered, u, me, h, t), out_sem.at[0, k % 2])

    def store_sum(k):
        u, h, t = steps[k]
        return pltpu.make_async_copy(sum_b.at[k % 2], tile(sums, u, 0, h, t), out_sem.at[1, k % 2])

    own_load(0).start()
    for copy in loads(0):
        copy.start()

    pl.semaphore_wait(barrier, 2)

    @pl.when(lax.rem(rep, 2) == 0)
    def _():
        @pl.loop(0, PAUSE * (ROWS // STRIP))
        def _(turn):
            at = pl.ds(pl.multiple_of(lax.rem(turn, ROWS // STRIP) * STRIP, STRIP), STRIP)
            m_b[1, at, :] = jnp.zeros((STRIP, COLS), jnp.float32)

    for i in range(3):
        for d in ways:
            first(d, i).start()
    for i in range(3):
        for d in ways:
            plain(d, i).start()

    for k, (d, u, t) in enumerate(adds):
        i, layer = units[u]
        if k + 1 < len(adds):
            own_load(k + 1).start()
        own_load(k).wait()
        if layer == t == 0:
            first(d, i).wait_recv()

        @pl.loop(0, ROWS // STRIP)
        def _(strip, d=d, i=i, layer=layer, t=t, k=k):
            at = pl.ds(pl.multiple_of(strip * STRIP, STRIP), STRIP)
            there = (d, layer, *lay[i].inside(t, strip))
            hop[i][there] = (hop[i][there].astype(jnp.float32) + own_b[k % 2, at, :].astype(jnp.float32)).astype(jnp.bfloat16)

        if layer == lay[i].layers - 1 and t == tiles - 1:
            added(d, i).start()

    def send_out(k):
        u, h, t = steps[k]
        store_new(k).wait()
        if h == 1 and t == tiles - 1:
            for d in ways:
                out(d, u).start()

    for k, (u, h, t) in enumerate(steps):
        s = k % 2
        i, layer = units[u]
        if k + 1 < len(steps):
            for copy in loads(k + 1):
                copy.start()
        for copy in loads(k):
            copy.wait()
        if layer == t == 0:
            for d in ways:
                (added if d == h else plain)(d, i).wait_recv()
        if k >= 2:
            store_sum(k - 2).wait()

        @pl.loop(0, ROWS // STRIP)
        def _(strip, s=s, i=i, layer=layer, h=h, t=t):
            at = pl.ds(pl.multiple_of(strip * STRIP, STRIP), STRIP)
            there = (h, layer, *lay[i].inside(t, strip))
            g = g_b[s, at, :].astype(jnp.float32) + got[i][(RIGHT, *there)].astype(jnp.float32)
            g = (g + got[i][(LEFT, *there)].astype(jnp.float32)).astype(jnp.bfloat16)
            sum_b[s, at, :] = g
            new_b[s, at, :] = adamw(w_b[s, at, :].astype(jnp.float32), m_b[s, at, :], v_b[s, at, :], g.astype(jnp.float32))[0]

        store_new(k).start()
        store_sum(k).start()
        if k >= 1:
            send_out(k - 1)
    end = len(steps) - 1
    send_out(end)
    store_sum(end - 1).wait()
    store_sum(end).wait()

    split = LATER * tiles - LAST
    later = [(u, d) for u in range(LATER) for d in ways]

    def take(k):
        u, d = later[k]
        i, layer = units[u]
        return pltpu.make_async_copy(part(gathered, u, came[d], d), hop[i].at[d, layer], own_sem.at[k % 2])

    def put(k, t):
        u, d = later[k]
        i, layer = units[u]
        src = hop[i].at[(d, layer, *lay[i].inside(t, None))]
        to_k = u * tiles + t
        dst = onward[d].at[to_k] if to_k < split else onward[2 + d].at[to_k - split]
        return pltpu.make_async_copy(src, dst, put_sem.at[k % 2, t])

    for i in range(3):
        for d in ways:
            added(d, i).wait_send()
    for k in range(len(later) + 2):
        if k < len(later):
            u, d = later[k]
            out(d, u).wait_recv()
            take(k).start()
        if 1 <= k <= len(later):
            take(k - 1).wait()
            for t in range(tiles):
                put(k - 1, t).start()
        if k >= 2:
            for t in range(tiles):
                put(k - 2, t).wait()
    for u in many[LATER:]:
        for d in ways:
            out(d, u).wait_recv()
            on(d, u).start()

    for d in ways:
        for i in range(3):
            first(d, i).wait_send()
            plain(d, i).wait_send()
        for u in many:
            out(d, u).wait_send()
            if u >= LATER:
                on(d, u).wait()


def settle(lay, *refs):
    ins, outs, buf, in_sem, out_sem = refs[:3], refs[3:6], refs[6], refs[7], refs[8]
    n = lax.axis_size("dp")
    me = lax.axis_index("dp")
    units = [(i, layer) for i in range(3) for layer in range(lay[i].layers)]
    tiles = [
        (i, layer, lax.rem(me + hops, n), h, t)
        for u, (i, layer) in enumerate(units)
        for hops in range(4)
        for h in range(2)
        for t in range(lay[i].tiles)
        if hops != 2 or u >= LATER
    ]

    def take(k):
        i, *where = tiles[k]
        return pltpu.make_async_copy(lay[i].tile(ins[i], *where), buf.at[k % FLIGHT], in_sem.at[k % FLIGHT])

    def put(k):
        i, *where = tiles[k]
        return pltpu.make_async_copy(buf.at[k % FLIGHT], lay[i].tile(outs[i], *where), out_sem.at[k % FLIGHT])

    lag = FLIGHT // 2
    for k in range(len(tiles) + lag):
        if k < len(tiles):
            if k >= FLIGHT:
                put(k - FLIGHT).wait()
            take(k).start()
        if k >= lag:
            take(k - lag).wait()
            put(k - lag).start()
    for k in range(len(tiles) - FLIGHT, len(tiles)):
        put(k).wait()


def spread(lay, first, *refs):
    brought, outs, sem = refs[:2], refs[5:8], refs[8]
    n = lax.axis_size("dp")
    across = lax.rem(lax.axis_index("dp") + 2, n)
    units = [(i, layer) for i in range(3) for layer in range(lay[i].layers)]
    tiles = lay[0].tiles
    copies = []
    for d in (RIGHT, LEFT):
        for k in range(brought[d].shape[0]):
            i, layer = units[(first + k) // tiles]
            dst = lay[i].tile(outs[i], layer, across, d, (first + k) % tiles)
            copies.append(pltpu.make_async_copy(brought[d].at[k], dst, sem.at[len(copies)]))
    for copy in copies:
        copy.start()
    for copy in copies:
        copy.wait()


def solution(mesh):
    def step(*arrays):
        terms, weights, m, v = (arrays[i : i + 3] for i in (0, 3, 6, 9))
        lay = [Lay(one.shape) for one in m]
        tiles = lay[0].tiles
        assert all(one.tiles == tiles for one in lay) and mesh.shape["dp"] == 4
        units = sum(one.layers for one in lay)
        anywhere = pl.BlockSpec(memory_space=pl.ANY)
        bf16 = jnp.bfloat16
        dma = pltpu.SemaphoreType.DMA
        res = pl.pallas_call(
            functools.partial(kernel, lay),
            out_shape=[jax.ShapeDtypeStruct(one.shape, bf16) for one in m]
            + [jax.ShapeDtypeStruct(one.shape, bf16) for one in weights]
            + [jax.ShapeDtypeStruct((LATER * tiles - LAST, ROWS, COLS), bf16)] * 2
            + [jax.ShapeDtypeStruct((LAST, ROWS, COLS), bf16)] * 2,
            in_specs=[anywhere] * 12,
            out_specs=[anywhere] * 10,
            scratch_shapes=[
                *(pltpu.VMEM((2, one.layers, *one.half), bf16) for one in lay),
                *(pltpu.VMEM((2, 2, one.layers, *one.half), bf16) for one in lay),
                pltpu.VMEM((2, ROWS, COLS), bf16),
                pltpu.VMEM((2, ROWS, COLS), bf16),
                pltpu.VMEM((2, ROWS, COLS), bf16),
                pltpu.VMEM((2, ROWS, COLS), jnp.float32),
                pltpu.VMEM((2, ROWS, COLS), jnp.float32),
                pltpu.VMEM((2, ROWS, COLS), bf16),
                pltpu.VMEM((2, ROWS, COLS), bf16),
                dma((2, 3)), dma((2, 3)),
                dma((2, 6)), dma((2, 6)),
                dma((2, units)), dma((2, units)),
                dma((2, units)), dma((2, units)),
                dma((2,)), dma((4, 2)), dma((2, 2)), dma((2, tiles)),
            ],
            compiler_params=pltpu.CompilerParams(collective_id=0, has_side_effects=True, vmem_limit_bytes=VMEM_LIMIT),
            name="sum_step_gather",
        )(*(t[0] for t in terms), *weights, *m, *v)
        sums, gathered, onward = res[:3], res[3:6], res[6:10]
        n = mesh.shape["dp"]
        brought = []
        for k in (0, 2):
            for x, hop in zip(onward[k : k + 2], (1, -1), strict=True):
                brought.append(lax.ppermute(x, "dp", [(i, (i + hop) % n) for i in range(n)]))
        size = sum(one.size for one in gathered)
        wholes = pl.pallas_call(
            functools.partial(settle, lay),
            out_shape=[jax.ShapeDtypeStruct(one.shape, one.dtype) for one in gathered],
            in_specs=[anywhere] * 3,
            out_specs=[anywhere] * 3,
            scratch_shapes=[pltpu.VMEM((FLIGHT, ROWS, COLS), bf16), dma((FLIGHT,)), dma((FLIGHT,))],
            compiler_params=pltpu.CompilerParams(vmem_limit_bytes=54 << 20),
            cost_estimate=pl.CostEstimate(flops=size * 40, bytes_accessed=4 * size, transcendentals=0),
            name="settle",
        )(*gathered)
        new_m, new_v = [], []
        for one_m, one_v, g in zip(m, v, sums, strict=True):
            g = g.astype(jnp.float32)
            new_m.append(0.9 * one_m + 0.1 * g)
            new_v.append(0.95 * one_v + 0.05 * g * g)
        for pair, first in ((brought[:2], 0), (brought[2:], LATER * tiles - LAST)):
            wholes = pl.pallas_call(
                functools.partial(spread, lay, first),
                out_shape=[jax.ShapeDtypeStruct(one.shape, one.dtype) for one in wholes],
                in_specs=[pl.BlockSpec(memory_space=pltpu.VMEM)] * 2 + [anywhere] * 3,
                out_specs=[anywhere] * 3,
                input_output_aliases={2: 0, 3: 1, 4: 2},
                scratch_shapes=[dma((2 * pair[0].shape[0],))],
                compiler_params=pltpu.CompilerParams(vmem_limit_bytes=24 << 20),
                name="spread",
            )(*pair, *wholes)
        return (*wholes, *new_m, *new_v)

    all_of, cut = P(None, None, None), P(None, "dp", None)
    return jax.shard_map(
        step,
        mesh=mesh,
        in_specs=(P(("rep", "dp"), None, None, None),) * 3 + (all_of,) * 3 + (cut,) * 6,
        out_specs=(P("rep", None, None),) * 3 + (P("rep", "dp", None),) * 6,
        check_vma=False,
    )
```

```python
import functools

import jax
import jax.numpy as jnp
from jax import lax
from jax.experimental import pallas as pl
from jax.experimental.pallas import tpu as pltpu
from jax.sharding import PartitionSpec as P


MESH = pl.DeviceIdType.MESH
ROWS, COLS = 256, 1024
RIGHT, LEFT = 0, 1
STRIP = 32
LATER = 4
LAST = 1
OWN = 8
AHEAD = 4
PAUSE = 144
FLIGHT = 32
VMEM_LIMIT = 67043328


def adamw(w, m, v, g):
    m = 0.9 * m + 0.1 * g
    v = 0.95 * v + 0.05 * g * g
    step = m * lax.rsqrt(v + 1e-8) + 0.1 * w
    return (w - 0.02 * step).astype(jnp.bfloat16), m, v


class Lay:
    def __init__(self, block):
        self.layers, self.rows, self.cols = block
        self.across = self.cols // COLS
        tiles = (self.rows // ROWS) * self.across
        assert self.rows % ROWS == 0 and self.cols % COLS == 0 and tiles % 2 == 0
        assert self.across == 1 or self.rows == ROWS
        self.tiles = tiles // 2
        self.half = (self.rows // 2, self.cols) if self.across == 1 else (self.rows, self.cols // 2)

    def of(self, ref, layer, owner, h):
        down, over = (h, 0) if self.across == 1 else (0, h)
        start = pl.multiple_of(owner * self.rows + down * self.half[0], ROWS)
        return ref.at[layer, pl.ds(start, self.half[0]), pl.ds(over * self.half[1], self.half[1])]

    def whole(self, ref, layer, owner):
        return ref.at[layer, pl.ds(pl.multiple_of(owner * self.rows, ROWS), self.rows)]

    def tile(self, ref, layer, owner, h, t):
        q = h * self.tiles + t
        start = pl.multiple_of(owner * self.rows + (q // self.across) * ROWS, ROWS)
        return ref.at[layer, pl.ds(start, ROWS), pl.ds((q % self.across) * COLS, COLS)]

    def inside(self, t, strip):
        down, over = (t, 0) if self.across == 1 else (0, t)
        if strip is None:
            return pl.ds(down * ROWS, ROWS), pl.ds(over * COLS, COLS)
        return pl.ds(pl.multiple_of(down * ROWS + strip * STRIP, STRIP), STRIP), pl.ds(over * COLS, COLS)


def kernel(lay, *refs):
    grads, weights, ms, vs, sums, gathered = (refs[i : i + 3] for i in range(0, 18, 3))
    onward, hop, got = refs[18:22], refs[22:25], refs[25:28]
    (
        own_b, g_b, w_b, m_b, v_b, sum_b, new_b,
        s1_send, s1_recv, s2_send, s2_recv, a1_send, a1_recv, a2_send, a2_recv,
        own_sem, in_sem, out_sem, put_sem,
    ) = refs[28:]
    n = lax.axis_size("dp")
    me = lax.axis_index("dp")
    rep = lax.axis_index("rep")
    right, left, across = lax.rem(me + 1, n), lax.rem(me + n - 1, n), lax.rem(me + 2, n)
    to = (right, left)
    came = (left, right)
    units = [(i, layer) for i in range(3) for layer in range(lay[i].layers)]
    many = range(len(units))
    tiles = lay[0].tiles
    ways = (RIGHT, LEFT)

    def remote(src, dst, sends, recvs, d, k):
        return pltpu.make_async_remote_copy(
            src_ref=src,
            dst_ref=dst,
            send_sem=sends.at[d, k],
            recv_sem=recvs.at[d, k],
            device_id=(rep, to[d]),
            device_id_type=MESH,
        )

    def part(arrays, u, owner, h):
        i, layer = units[u]
        return lay[i].of(arrays[i], layer, owner, h)

    def tile(arrays, u, owner, h, t):
        i, layer = units[u]
        return lay[i].tile(arrays[i], layer, owner, h, t)

    def first(d, u):
        i, layer = units[u]
        return remote(part(grads, u, across, d), hop[i].at[d, layer], s1_send, s1_recv, d, u)

    def plain(d, u):
        i, layer = units[u]
        return remote(part(grads, u, to[d], 1 - d), got[i].at[d, 1 - d, layer], s2_send, s2_recv, d, 2 * u + 1 - d)

    def added(d, u):
        i, layer = units[u]
        return remote(hop[i].at[d, layer], got[i].at[d, d, layer], s2_send, s2_recv, d, 2 * u + d)

    def out(d, u):
        i, layer = units[u]
        src = lay[i].whole(gathered[i], layer, me)
        return remote(src, src, a1_send, a1_recv, d, u)

    def on(d, u):
        src = part(gathered, u, came[d], d)
        return remote(src, src, a2_send, a2_recv, d, u)

    barrier = pltpu.get_barrier_semaphore()
    for device in to:
        pl.semaphore_signal(barrier, inc=1, device_id=(rep, device), device_id_type=MESH)

    adds = [(d, u, t) for u in many for d in ways for t in range(tiles)]
    steps = [(u, h, t) for u in many for h in range(2) for t in range(tiles)]

    def own_load(k):
        d, u, t = adds[k]
        return pltpu.make_async_copy(tile(grads, u, to[d], d, t), own_b.at[k % OWN], own_sem.at[k % OWN])

    def loads(k):
        u, h, t = steps[k]
        s = k % AHEAD
        pairs = ((tile(grads, u, me, h, t), g_b), (tile(weights, u, me, h, t), w_b), (tile(ms, u, 0, h, t), m_b), (tile(vs, u, 0, h, t), v_b))
        return [pltpu.make_async_copy(src, dst.at[s], in_sem.at[a, s]) for a, (src, dst) in enumerate(pairs)]

    def store_new(k):
        u, h, t = steps[k]
        return pltpu.make_async_copy(new_b.at[k % 2], tile(gathered, u, me, h, t), out_sem.at[0, k % 2])

    def store_sum(k):
        u, h, t = steps[k]
        return pltpu.make_async_copy(sum_b.at[k % 2], tile(sums, u, 0, h, t), out_sem.at[1, k % 2])

    for k in range(OWN):
        own_load(k).start()
    for k in range(AHEAD):
        for copy in loads(k):
            copy.start()

    pl.semaphore_wait(barrier, 2)

    @pl.when(lax.rem(rep, 2) == 0)
    def _():
        @pl.loop(0, PAUSE * (ROWS // STRIP))
        def _(turn):
            at = pl.ds(pl.multiple_of(lax.rem(turn, ROWS // STRIP) * STRIP, STRIP), STRIP)
            sum_b[0, at, :] = jnp.zeros((STRIP, COLS), jnp.bfloat16)

    for u in many:
        for d in ways:
            first(d, u).start()
    for u in many:
        for d in ways:
            plain(d, u).start()

    for k, (d, u, t) in enumerate(adds):
        i, layer = units[u]
        if t == 0:
            first(d, u).wait_recv()
        own_load(k).wait()

        @pl.loop(0, ROWS // STRIP)
        def _(strip, d=d, i=i, layer=layer, t=t, k=k):
            at = pl.ds(pl.multiple_of(strip * STRIP, STRIP), STRIP)
            there = (d, layer, *lay[i].inside(t, strip))
            hop[i][there] = (hop[i][there].astype(jnp.float32) + own_b[k % OWN, at, :].astype(jnp.float32)).astype(jnp.bfloat16)

        if t == tiles - 1:
            added(d, u).start()
        if k + OWN < len(adds):
            own_load(k + OWN).start()

    def send_out(k):
        u, h, t = steps[k]
        store_new(k).wait()
        if h == 1 and t == tiles - 1:
            for d in ways:
                out(d, u).start()

    for k, (u, h, t) in enumerate(steps):
        s = k % 2
        i, layer = units[u]
        if t == 0:
            for d in ways:
                (added if d == h else plain)(d, u).wait_recv()
        for copy in loads(k):
            copy.wait()
        if k >= 2:
            store_sum(k - 2).wait()

        @pl.loop(0, ROWS // STRIP)
        def _(strip, s=s, a=k % AHEAD, i=i, layer=layer, h=h, t=t):
            at = pl.ds(pl.multiple_of(strip * STRIP, STRIP), STRIP)
            there = (h, layer, *lay[i].inside(t, strip))
            g = g_b[a, at, :].astype(jnp.float32) + got[i][(RIGHT, *there)].astype(jnp.float32)
            g = (g + got[i][(LEFT, *there)].astype(jnp.float32)).astype(jnp.bfloat16)
            sum_b[s, at, :] = g
            new_b[s, at, :] = adamw(w_b[a, at, :].astype(jnp.float32), m_b[a, at, :], v_b[a, at, :], g.astype(jnp.float32))[0]

        store_new(k).start()
        store_sum(k).start()
        if k + AHEAD < len(steps):
            for copy in loads(k + AHEAD):
                copy.start()
        if k >= 1:
            send_out(k - 1)
    end = len(steps) - 1
    send_out(end)
    store_sum(end - 1).wait()
    store_sum(end).wait()

    split = LATER * tiles - LAST
    later = [(u, d) for u in range(LATER) for d in ways]

    def take(k):
        u, d = later[k]
        i, layer = units[u]
        return pltpu.make_async_copy(part(gathered, u, came[d], d), hop[i].at[d, layer], own_sem.at[k % 2])

    def put(k, t):
        u, d = later[k]
        i, layer = units[u]
        src = hop[i].at[(d, layer, *lay[i].inside(t, None))]
        to_k = u * tiles + t
        dst = onward[d].at[to_k] if to_k < split else onward[2 + d].at[to_k - split]
        return pltpu.make_async_copy(src, dst, put_sem.at[k % 2, t])

    for u in many:
        for d in ways:
            added(d, u).wait_send()
    for k in range(len(later) + 2):
        if k < len(later):
            u, d = later[k]
            out(d, u).wait_recv()
            take(k).start()
        if 1 <= k <= len(later):
            take(k - 1).wait()
            for t in range(tiles):
                put(k - 1, t).start()
        if k >= 2:
            for t in range(tiles):
                put(k - 2, t).wait()
    for u in many[LATER:]:
        for d in ways:
            out(d, u).wait_recv()
            on(d, u).start()

    for d in ways:
        for u in many:
            first(d, u).wait_send()
            plain(d, u).wait_send()
            out(d, u).wait_send()
            if u >= LATER:
                on(d, u).wait()


def settle(lay, *refs):
    ins, outs, buf, in_sem, out_sem = refs[:3], refs[3:6], refs[6], refs[7], refs[8]
    n = lax.axis_size("dp")
    me = lax.axis_index("dp")
    units = [(i, layer) for i in range(3) for layer in range(lay[i].layers)]
    tiles = [
        (i, layer, lax.rem(me + hops, n), h, t)
        for u, (i, layer) in enumerate(units)
        for hops in range(4)
        for h in range(2)
        for t in range(lay[i].tiles)
        if hops != 2 or u >= LATER
    ]

    def take(k):
        i, *where = tiles[k]
        return pltpu.make_async_copy(lay[i].tile(ins[i], *where), buf.at[k % FLIGHT], in_sem.at[k % FLIGHT])

    def put(k):
        i, *where = tiles[k]
        return pltpu.make_async_copy(buf.at[k % FLIGHT], lay[i].tile(outs[i], *where), out_sem.at[k % FLIGHT])

    lag = FLIGHT // 2
    for k in range(len(tiles) + lag):
        if k < len(tiles):
            if k >= FLIGHT:
                put(k - FLIGHT).wait()
            take(k).start()
        if k >= lag:
            take(k - lag).wait()
            put(k - lag).start()
    for k in range(len(tiles) - FLIGHT, len(tiles)):
        put(k).wait()


def spread(lay, first, *refs):
    brought, outs, sem = refs[:2], refs[5:8], refs[8]
    n = lax.axis_size("dp")
    across = lax.rem(lax.axis_index("dp") + 2, n)
    units = [(i, layer) for i in range(3) for layer in range(lay[i].layers)]
    tiles = lay[0].tiles
    copies = []
    for d in (RIGHT, LEFT):
        for k in range(brought[d].shape[0]):
            i, layer = units[(first + k) // tiles]
            dst = lay[i].tile(outs[i], layer, across, d, (first + k) % tiles)
            copies.append(pltpu.make_async_copy(brought[d].at[k], dst, sem.at[len(copies)]))
    for copy in copies:
        copy.start()
    for copy in copies:
        copy.wait()


def solution(mesh):
    def step(*arrays):
        terms, weights, m, v = (arrays[i : i + 3] for i in (0, 3, 6, 9))
        lay = [Lay(one.shape) for one in m]
        tiles = lay[0].tiles
        assert all(one.tiles == tiles for one in lay) and mesh.shape["dp"] == 4
        units = sum(one.layers for one in lay)
        anywhere = pl.BlockSpec(memory_space=pl.ANY)
        bf16 = jnp.bfloat16
        dma = pltpu.SemaphoreType.DMA
        res = pl.pallas_call(
            functools.partial(kernel, lay),
            out_shape=[jax.ShapeDtypeStruct(one.shape, bf16) for one in m]
            + [jax.ShapeDtypeStruct(one.shape, bf16) for one in weights]
            + [jax.ShapeDtypeStruct((LATER * tiles - LAST, ROWS, COLS), bf16)] * 2
            + [jax.ShapeDtypeStruct((LAST, ROWS, COLS), bf16)] * 2,
            in_specs=[anywhere] * 12,
            out_specs=[anywhere] * 10,
            scratch_shapes=[
                *(pltpu.VMEM((2, one.layers, *one.half), bf16) for one in lay),
                *(pltpu.VMEM((2, 2, one.layers, *one.half), bf16) for one in lay),
                pltpu.VMEM((OWN, ROWS, COLS), bf16),
                pltpu.VMEM((AHEAD, ROWS, COLS), bf16),
                pltpu.VMEM((AHEAD, ROWS, COLS), bf16),
                pltpu.VMEM((AHEAD, ROWS, COLS), jnp.float32),
                pltpu.VMEM((AHEAD, ROWS, COLS), jnp.float32),
                pltpu.VMEM((2, ROWS, COLS), bf16),
                pltpu.VMEM((2, ROWS, COLS), bf16),
                dma((2, units)), dma((2, units)),
                dma((2, 2 * units)), dma((2, 2 * units)),
                dma((2, units)), dma((2, units)),
                dma((2, units)), dma((2, units)),
                dma((OWN,)), dma((4, AHEAD)), dma((2, 2)), dma((2, tiles)),
            ],
            compiler_params=pltpu.CompilerParams(collective_id=0, has_side_effects=True, vmem_limit_bytes=VMEM_LIMIT),
            name="sum_step_gather",
        )(*(t[0] for t in terms), *weights, *m, *v)
        sums, gathered, onward = res[:3], res[3:6], res[6:10]
        n = mesh.shape["dp"]
        brought = []
        for k in (0, 2):
            for x, hop in zip(onward[k : k + 2], (1, -1), strict=True):
                brought.append(lax.ppermute(x, "dp", [(i, (i + hop) % n) for i in range(n)]))
        size = sum(one.size for one in gathered)
        wholes = pl.pallas_call(
            functools.partial(settle, lay),
            out_shape=[jax.ShapeDtypeStruct(one.shape, one.dtype) for one in gathered],
            in_specs=[anywhere] * 3,
            out_specs=[anywhere] * 3,
            scratch_shapes=[pltpu.VMEM((FLIGHT, ROWS, COLS), bf16), dma((FLIGHT,)), dma((FLIGHT,))],
            compiler_params=pltpu.CompilerParams(vmem_limit_bytes=54 << 20),
            cost_estimate=pl.CostEstimate(flops=size * 40, bytes_accessed=4 * size, transcendentals=0),
            name="settle",
        )(*gathered)
        new_m, new_v = [], []
        for one_m, one_v, g in zip(m, v, sums, strict=True):
            g = g.astype(jnp.float32)
            new_m.append(0.9 * one_m + 0.1 * g)
            new_v.append(0.95 * one_v + 0.05 * g * g)
        for pair, first in ((brought[:2], 0), (brought[2:], LATER * tiles - LAST)):
            wholes = pl.pallas_call(
                functools.partial(spread, lay, first),
                out_shape=[jax.ShapeDtypeStruct(one.shape, one.dtype) for one in wholes],
                in_specs=[pl.BlockSpec(memory_space=pltpu.VMEM)] * 2 + [anywhere] * 3,
                out_specs=[anywhere] * 3,
                input_output_aliases={2: 0, 3: 1, 4: 2},
                scratch_shapes=[dma((2 * pair[0].shape[0],))],
                compiler_params=pltpu.CompilerParams(vmem_limit_bytes=24 << 20),
                name="spread",
            )(*pair, *wholes)
        return (*wholes, *new_m, *new_v)

    all_of, cut = P(None, None, None), P(None, "dp", None)
    return jax.shard_map(
        step,
        mesh=mesh,
        in_specs=(P(("rep", "dp"), None, None, None),) * 3 + (all_of,) * 3 + (cut,) * 6,
        out_specs=(P("rep", None, None),) * 3 + (P("rep", "dp", None),) * 6,
        check_vma=False,
    )
```

```python
import functools

import jax
import jax.numpy as jnp
from jax import lax
from jax.experimental import pallas as pl
from jax.experimental.pallas import tpu as pltpu
from jax.sharding import PartitionSpec as P


MESH = pl.DeviceIdType.MESH
ROWS, COLS = 256, 1024
RIGHT, LEFT = 0, 1
STRIP = 32
LATER = 4
CUT = 192
OWN = 8
AHEAD = 4
PAUSE = 144
FLIGHT = 32
VMEM_LIMIT = 67043328


def adamw(w, m, v, g):
    m = 0.9 * m + 0.1 * g
    v = 0.95 * v + 0.05 * g * g
    step = m * lax.rsqrt(v + 1e-8) + 0.1 * w
    return (w - 0.02 * step).astype(jnp.bfloat16), m, v


class Lay:
    def __init__(self, block):
        self.layers, self.rows, self.cols = block
        self.across = self.cols // COLS
        tiles = (self.rows // ROWS) * self.across
        assert self.rows % ROWS == 0 and self.cols % COLS == 0 and tiles % 2 == 0
        assert self.across == 1 or self.rows == ROWS
        self.tiles = tiles // 2
        self.half = (self.rows // 2, self.cols) if self.across == 1 else (self.rows, self.cols // 2)

    def of(self, ref, layer, owner, h):
        down, over = (h, 0) if self.across == 1 else (0, h)
        start = pl.multiple_of(owner * self.rows + down * self.half[0], ROWS)
        return ref.at[layer, pl.ds(start, self.half[0]), pl.ds(over * self.half[1], self.half[1])]

    def whole(self, ref, layer, owner):
        return ref.at[layer, pl.ds(pl.multiple_of(owner * self.rows, ROWS), self.rows)]

    def tile(self, ref, layer, owner, h, t):
        q = h * self.tiles + t
        start = pl.multiple_of(owner * self.rows + (q // self.across) * ROWS, ROWS)
        return ref.at[layer, pl.ds(start, ROWS), pl.ds((q % self.across) * COLS, COLS)]

    def inside(self, t, strip):
        down, over = (t, 0) if self.across == 1 else (0, t)
        if strip is None:
            return pl.ds(down * ROWS, ROWS), pl.ds(over * COLS, COLS)
        return pl.ds(pl.multiple_of(down * ROWS + strip * STRIP, STRIP), STRIP), pl.ds(over * COLS, COLS)


def kernel(lay, *refs):
    grads, weights, ms, vs, sums, gathered = (refs[i : i + 3] for i in range(0, 18, 3))
    onward, hop, got = refs[18:24], refs[24:27], refs[27:30]
    (
        own_b, g_b, w_b, m_b, v_b, sum_b, new_b,
        s1_send, s1_recv, s2_send, s2_recv, a1_send, a1_recv, a2_send, a2_recv,
        own_sem, in_sem, out_sem, put_sem,
    ) = refs[30:]
    n = lax.axis_size("dp")
    me = lax.axis_index("dp")
    rep = lax.axis_index("rep")
    right, left, across = lax.rem(me + 1, n), lax.rem(me + n - 1, n), lax.rem(me + 2, n)
    to = (right, left)
    came = (left, right)
    units = [(i, layer) for i in range(3) for layer in range(lay[i].layers)]
    many = range(len(units))
    tiles = lay[0].tiles
    ways = (RIGHT, LEFT)

    def remote(src, dst, sends, recvs, d, k):
        return pltpu.make_async_remote_copy(
            src_ref=src,
            dst_ref=dst,
            send_sem=sends.at[d, k],
            recv_sem=recvs.at[d, k],
            device_id=(rep, to[d]),
            device_id_type=MESH,
        )

    def part(arrays, u, owner, h):
        i, layer = units[u]
        return lay[i].of(arrays[i], layer, owner, h)

    def tile(arrays, u, owner, h, t):
        i, layer = units[u]
        return lay[i].tile(arrays[i], layer, owner, h, t)

    def first(d, u):
        i, layer = units[u]
        return remote(part(grads, u, across, d), hop[i].at[d, layer], s1_send, s1_recv, d, u)

    def plain(d, u):
        i, layer = units[u]
        return remote(part(grads, u, to[d], 1 - d), got[i].at[d, 1 - d, layer], s2_send, s2_recv, d, 2 * u + 1 - d)

    def added(d, u):
        i, layer = units[u]
        return remote(hop[i].at[d, layer], got[i].at[d, d, layer], s2_send, s2_recv, d, 2 * u + d)

    def out(d, u):
        i, layer = units[u]
        src = lay[i].whole(gathered[i], layer, me)
        return remote(src, src, a1_send, a1_recv, d, u)

    def on(d, u):
        src = part(gathered, u, came[d], d)
        return remote(src, src, a2_send, a2_recv, d, u)

    barrier = pltpu.get_barrier_semaphore()
    for device in to:
        pl.semaphore_signal(barrier, inc=1, device_id=(rep, device), device_id_type=MESH)

    adds = [(d, u, t) for u in many for d in ways for t in range(tiles)]
    steps = [(u, h, t) for u in many for h in range(2) for t in range(tiles)]

    def own_load(k):
        d, u, t = adds[k]
        return pltpu.make_async_copy(tile(grads, u, to[d], d, t), own_b.at[k % OWN], own_sem.at[k % OWN])

    def loads(k):
        u, h, t = steps[k]
        s = k % AHEAD
        pairs = ((tile(grads, u, me, h, t), g_b), (tile(weights, u, me, h, t), w_b), (tile(ms, u, 0, h, t), m_b), (tile(vs, u, 0, h, t), v_b))
        return [pltpu.make_async_copy(src, dst.at[s], in_sem.at[a, s]) for a, (src, dst) in enumerate(pairs)]

    def store_new(k):
        u, h, t = steps[k]
        return pltpu.make_async_copy(new_b.at[k % 2], tile(gathered, u, me, h, t), out_sem.at[0, k % 2])

    def store_sum(k):
        u, h, t = steps[k]
        return pltpu.make_async_copy(sum_b.at[k % 2], tile(sums, u, 0, h, t), out_sem.at[1, k % 2])

    for k in range(OWN):
        own_load(k).start()
    for k in range(AHEAD):
        for copy in loads(k):
            copy.start()

    pl.semaphore_wait(barrier, 2)

    @pl.when(lax.rem(rep, 2) == 0)
    def _():
        @pl.loop(0, PAUSE * (ROWS // STRIP))
        def _(turn):
            at = pl.ds(pl.multiple_of(lax.rem(turn, ROWS // STRIP) * STRIP, STRIP), STRIP)
            sum_b[0, at, :] = jnp.zeros((STRIP, COLS), jnp.bfloat16)

    for u in many:
        for d in ways:
            first(d, u).start()
    for u in many:
        for d in ways:
            plain(d, u).start()

    for k, (d, u, t) in enumerate(adds):
        i, layer = units[u]
        if t == 0:
            first(d, u).wait_recv()
        own_load(k).wait()

        @pl.loop(0, ROWS // STRIP)
        def _(strip, d=d, i=i, layer=layer, t=t, k=k):
            at = pl.ds(pl.multiple_of(strip * STRIP, STRIP), STRIP)
            there = (d, layer, *lay[i].inside(t, strip))
            hop[i][there] = (hop[i][there].astype(jnp.float32) + own_b[k % OWN, at, :].astype(jnp.float32)).astype(jnp.bfloat16)

        if t == tiles - 1:
            added(d, u).start()
        if k + OWN < len(adds):
            own_load(k + OWN).start()

    def send_out(k):
        u, h, t = steps[k]
        store_new(k).wait()
        if h == 1 and t == tiles - 1:
            for d in ways:
                out(d, u).start()

    for k, (u, h, t) in enumerate(steps):
        s = k % 2
        i, layer = units[u]
        if t == 0:
            for d in ways:
                (added if d == h else plain)(d, u).wait_recv()
        for copy in loads(k):
            copy.wait()
        if k >= 2:
            store_sum(k - 2).wait()

        @pl.loop(0, ROWS // STRIP)
        def _(strip, s=s, a=k % AHEAD, i=i, layer=layer, h=h, t=t):
            at = pl.ds(pl.multiple_of(strip * STRIP, STRIP), STRIP)
            there = (h, layer, *lay[i].inside(t, strip))
            g = g_b[a, at, :].astype(jnp.float32) + got[i][(RIGHT, *there)].astype(jnp.float32)
            g = (g + got[i][(LEFT, *there)].astype(jnp.float32)).astype(jnp.bfloat16)
            sum_b[s, at, :] = g
            new_b[s, at, :] = adamw(w_b[a, at, :].astype(jnp.float32), m_b[a, at, :], v_b[a, at, :], g.astype(jnp.float32))[0]

        store_new(k).start()
        store_sum(k).start()
        if k + AHEAD < len(steps):
            for copy in loads(k + AHEAD):
                copy.start()
        if k >= 1:
            send_out(k - 1)
    end = len(steps) - 1
    send_out(end)
    store_sum(end - 1).wait()
    store_sum(end).wait()

    later = [(u, d) for u in range(LATER) for d in ways]

    def take(k):
        u, d = later[k]
        i, layer = units[u]
        return pltpu.make_async_copy(part(gathered, u, came[d], d), hop[i].at[d, layer], own_sem.at[k % 2])

    def puts(k):
        u, d = later[k]
        i, layer = units[u]
        copies = []
        for t in range(tiles):
            src = hop[i].at[(d, layer, *lay[i].inside(t, None))]
            if u * tiles + t < LATER * tiles - 1:
                copies.append((src, onward[d].at[u * tiles + t]))
            else:
                copies.append((src.at[pl.ds(0, CUT), :], onward[2 + d].at[0]))
                copies.append((src.at[pl.ds(CUT, ROWS - CUT), :], onward[4 + d].at[0]))
        return [pltpu.make_async_copy(*copy, put_sem.at[k % 2, c]) for c, copy in enumerate(copies)]

    for u in many:
        for d in ways:
            added(d, u).wait_send()
    for k in range(len(later) + 2):
        if k < len(later):
            u, d = later[k]
            out(d, u).wait_recv()
            take(k).start()
        if 1 <= k <= len(later):
            take(k - 1).wait()
            for copy in puts(k - 1):
                copy.start()
        if k >= 2:
            for copy in puts(k - 2):
                copy.wait()
    for u in many[LATER:]:
        for d in ways:
            out(d, u).wait_recv()
            on(d, u).start()

    for d in ways:
        for u in many:
            first(d, u).wait_send()
            plain(d, u).wait_send()
            out(d, u).wait_send()
            if u >= LATER:
                on(d, u).wait()


def settle(lay, *refs):
    ins, outs, buf, in_sem, out_sem = refs[:3], refs[3:6], refs[6], refs[7], refs[8]
    n = lax.axis_size("dp")
    me = lax.axis_index("dp")
    units = [(i, layer) for i in range(3) for layer in range(lay[i].layers)]
    tiles = [
        (i, layer, lax.rem(me + hops, n), h, t)
        for u, (i, layer) in enumerate(units)
        for hops in range(4)
        for h in range(2)
        for t in range(lay[i].tiles)
        if hops != 2 or u >= LATER
    ]

    def take(k):
        i, *where = tiles[k]
        return pltpu.make_async_copy(lay[i].tile(ins[i], *where), buf.at[k % FLIGHT], in_sem.at[k % FLIGHT])

    def put(k):
        i, *where = tiles[k]
        return pltpu.make_async_copy(buf.at[k % FLIGHT], lay[i].tile(outs[i], *where), out_sem.at[k % FLIGHT])

    lag = FLIGHT - FLIGHT // 4
    for k in range(len(tiles) + lag):
        if k < len(tiles):
            if k >= FLIGHT:
                put(k - FLIGHT).wait()
            take(k).start()
        if k >= lag:
            take(k - lag).wait()
            put(k - lag).start()
    for k in range(len(tiles) - FLIGHT, len(tiles)):
        put(k).wait()


def spread(lay, first, start, *refs):
    brought, outs, sem = refs[:2], refs[5:8], refs[8]
    n = lax.axis_size("dp")
    across = lax.rem(lax.axis_index("dp") + 2, n)
    units = [(i, layer) for i in range(3) for layer in range(lay[i].layers)]
    tiles = lay[0].tiles
    copies = []
    for d in (RIGHT, LEFT):
        for k in range(brought[d].shape[0]):
            i, layer = units[(first + k) // tiles]
            dst = lay[i].tile(outs[i], layer, across, d, (first + k) % tiles)
            dst = dst.at[pl.ds(start, brought[d].shape[1]), :]
            copies.append(pltpu.make_async_copy(brought[d].at[k], dst, sem.at[len(copies)]))
    for copy in copies:
        copy.start()
    for copy in copies:
        copy.wait()


def solution(mesh):
    def step(*arrays):
        terms, weights, m, v = (arrays[i : i + 3] for i in (0, 3, 6, 9))
        lay = [Lay(one.shape) for one in m]
        tiles = lay[0].tiles
        assert all(one.tiles == tiles for one in lay) and mesh.shape["dp"] == 4
        units = sum(one.layers for one in lay)
        anywhere = pl.BlockSpec(memory_space=pl.ANY)
        bf16 = jnp.bfloat16
        dma = pltpu.SemaphoreType.DMA
        res = pl.pallas_call(
            functools.partial(kernel, lay),
            out_shape=[jax.ShapeDtypeStruct(one.shape, bf16) for one in m]
            + [jax.ShapeDtypeStruct(one.shape, bf16) for one in weights]
            + [jax.ShapeDtypeStruct((LATER * tiles - 1, ROWS, COLS), bf16)] * 2
            + [jax.ShapeDtypeStruct((1, CUT, COLS), bf16)] * 2
            + [jax.ShapeDtypeStruct((1, ROWS - CUT, COLS), bf16)] * 2,
            in_specs=[anywhere] * 12,
            out_specs=[anywhere] * 12,
            scratch_shapes=[
                *(pltpu.VMEM((2, one.layers, *one.half), bf16) for one in lay),
                *(pltpu.VMEM((2, 2, one.layers, *one.half), bf16) for one in lay),
                pltpu.VMEM((OWN, ROWS, COLS), bf16),
                pltpu.VMEM((AHEAD, ROWS, COLS), bf16),
                pltpu.VMEM((AHEAD, ROWS, COLS), bf16),
                pltpu.VMEM((AHEAD, ROWS, COLS), jnp.float32),
                pltpu.VMEM((AHEAD, ROWS, COLS), jnp.float32),
                pltpu.VMEM((2, ROWS, COLS), bf16),
                pltpu.VMEM((2, ROWS, COLS), bf16),
                dma((2, units)), dma((2, units)),
                dma((2, 2 * units)), dma((2, 2 * units)),
                dma((2, units)), dma((2, units)),
                dma((2, units)), dma((2, units)),
                dma((OWN,)), dma((4, AHEAD)), dma((2, 2)), dma((2, tiles + 1)),
            ],
            compiler_params=pltpu.CompilerParams(collective_id=0, has_side_effects=True, vmem_limit_bytes=VMEM_LIMIT),
            name="sum_step_gather",
        )(*(t[0] for t in terms), *weights, *m, *v)
        sums, gathered, onward = res[:3], res[3:6], res[6:12]
        n = mesh.shape["dp"]
        brought = []
        for k in (0, 2, 4):
            for x, hop in zip(onward[k : k + 2], (1, -1), strict=True):
                brought.append(lax.ppermute(x, "dp", [(i, (i + hop) % n) for i in range(n)]))
        size = sum(one.size for one in gathered)
        wholes = pl.pallas_call(
            functools.partial(settle, lay),
            out_shape=[jax.ShapeDtypeStruct(one.shape, one.dtype) for one in gathered],
            in_specs=[anywhere] * 3,
            out_specs=[anywhere] * 3,
            scratch_shapes=[pltpu.VMEM((FLIGHT, ROWS, COLS), bf16), dma((FLIGHT,)), dma((FLIGHT,))],
            compiler_params=pltpu.CompilerParams(vmem_limit_bytes=54 << 20),
            cost_estimate=pl.CostEstimate(flops=size * 40, bytes_accessed=4 * size, transcendentals=0),
            name="settle",
        )(*gathered)
        new_m, new_v = [], []
        for one_m, one_v, g in zip(m, v, sums, strict=True):
            g = g.astype(jnp.float32)
            new_m.append(0.9 * one_m + 0.1 * g)
            new_v.append(0.95 * one_v + 0.05 * g * g)
        for pair, first, start in ((brought[:2], 0, 0), (brought[2:4], LATER * tiles - 1, 0), (brought[4:], LATER * tiles - 1, CUT)):
            wholes = pl.pallas_call(
                functools.partial(spread, lay, first, start),
                out_shape=[jax.ShapeDtypeStruct(one.shape, one.dtype) for one in wholes],
                in_specs=[pl.BlockSpec(memory_space=pltpu.VMEM)] * 2 + [anywhere] * 3,
                out_specs=[anywhere] * 3,
                input_output_aliases={2: 0, 3: 1, 4: 2},
                scratch_shapes=[dma((2 * pair[0].shape[0],))],
                compiler_params=pltpu.CompilerParams(vmem_limit_bytes=24 << 20),
                name="spread",
            )(*pair, *wholes)
        return (*wholes, *new_m, *new_v)

    all_of, cut = P(None, None, None), P(None, "dp", None)
    return jax.shard_map(
        step,
        mesh=mesh,
        in_specs=(P(("rep", "dp"), None, None, None),) * 3 + (all_of,) * 3 + (cut,) * 6,
        out_specs=(P("rep", None, None),) * 3 + (P("rep", "dp", None),) * 6,
        check_vma=False,
    )
```
